128 devices in a mesh: section: 32 (over y, z, core), tensor: 4 (over x).
Axes of the slice: x: 4, y: 4, z: 4, core: 2. Of those that a mesh axis runs over, the one named last changes fastest.
Arguments:
- section_input: bfloat16 [32, 512, 4096], P('section', 'tensor'), may hold values from -6 to 6
- history: bfloat16 [32, 7, 512, 4096], P('section', None, 'tensor'), may hold values from -6 to 6
- query_weight: bfloat16 [32, 4096, 3072], P('section', None, 'tensor'), may hold values from -0.4 to 0.4
- key_weight: bfloat16 [32, 4096, 512], P('section', None, 'tensor'), may hold values from -0.4 to 0.4
- value_weight: bfloat16 [32, 4096, 512], P('section', None, 'tensor'), may hold values from -0.09375 to 0.09375
- output_weight: bfloat16 [32, 3072, 4096], P('section', 'tensor'), may hold values from -0.5 to 0.5
- mix_weights: float32 [32, 8], replicated, may hold values from 0.2 to 0.6
Outputs:
- next_input: bfloat16 [32, 512, 4096], P('section', 'tensor')
The draws below stay inside these ranges and needn't reach their ends.
All inputs are finite; a program needn't handle non-finite values.
Results may differ from the reference program's by a relative error of at most 0.013.
The reference program's roundings to bfloat16 on the way count: a program that leaves them out, or rounds other values in their place, can miss the bound.
Values may be sent and summed in bfloat16 or wider, within the bound.
No kernel may reach another device: no remote copies, remote signals or barrier semaphores. Data moves between devices by JAX's collectives and lax.ppermute only.
A program may use at most 128 MiB of HBM per device.

```python
import math
import jax
import jax.numpy as jnp
from jax import lax

D = 4096
HEADS = 48
KV_HEADS = 8
HEAD_DIM = 64
DILATION_STRIDE = 4
SEQ = 512
HIST = 7
N_SECTION = 32
N_TENSOR = 4


def draw_query_weight(key, part):
    entries = jax.random.normal(jax.random.fold_in(key, 11), (N_SECTION, D, HEADS * HEAD_DIM), jnp.float32) / jnp.sqrt(jnp.float32(D))
    return jnp.clip(entries, -0.39, 0.39).astype(jnp.bfloat16)


def draw_key_weight(key, part):
    entries = jax.random.normal(jax.random.fold_in(key, 13), (N_SECTION, D, KV_HEADS * HEAD_DIM), jnp.float32) / jnp.sqrt(jnp.float32(D))
    return jnp.clip(entries, -0.39, 0.39).astype(jnp.bfloat16)


def steps_of(rng, extent, shards, low, high):
    level, own = 1.0, jax.random.fold_in(rng, 6)
    for dim, shards_of in shards:
        heights = jnp.exp(jax.random.uniform(jax.random.fold_in(own, dim), (shards_of,), jnp.float32, low / len(shards), high / len(shards)))
        level = level * jnp.repeat(heights, extent[dim] // shards_of).reshape([-1 if axis == dim else 1 for axis in range(len(extent))])
    return level


def noise(key, shape, spread, reach, shards=(), kind=jnp.bfloat16):
    factor_of = steps_of(key, shape, shards, -0.22, 0.18) if shards else 1.0
    result = jax.random.normal(key, shape, jnp.float32) * spread * factor_of
    return jnp.minimum(jnp.maximum(result, -reach), reach).astype(kind)


def setup_inputs(seed: int = 0) -> dict:
    seeds = jax.random.split(jax.random.key(seed), 8)
    return {
        "section_input": noise(seeds[0], (N_SECTION, SEQ, D), 1.0, 6.0, ((0, 32), (1, 4))),
        "history": noise(seeds[1], (N_SECTION, HIST, SEQ, D), 1.0, 6.0, ((0, 32), (2, 4))),
        "query_weight": draw_query_weight(jax.random.fold_in(seeds[7], 71), 0),
        "key_weight": draw_key_weight(jax.random.fold_in(seeds[7], 71), 0),
        "value_weight": noise(seeds[4], (N_SECTION, D, KV_HEADS * HEAD_DIM), D ** -0.5, 0.09375, ((0, 32), (2, 4))),
        "output_weight": noise(seeds[5], (N_SECTION, HEADS * HEAD_DIM, D), 0.08, 0.5, ((0, 32), (1, 4))),
        "mix_weights": jnp.clip(jax.random.uniform(seeds[6], (N_SECTION, HIST + 1), jnp.float32, 0.2, 0.6), 0.2, 0.6),
    }


def normalize(token_rows):
    values = token_rows.astype(jnp.float32)
    inv_scale = lax.rsqrt(lax.optimization_barrier(jnp.mean(values * values, axis=-1, keepdims=True)) + 1e-05)
    return (values * inv_scale).astype(jnp.bfloat16)

def one_section(operands):
    token_rows, query_part, key_part, value_part, output_part = operands
    seq_len = token_rows.shape[0]
    normed = normalize(token_rows)
    query_rows = jnp.dot(normed, query_part, preferred_element_type=jnp.float32).astype(jnp.bfloat16)
    key_rows = jnp.dot(normed, key_part, preferred_element_type=jnp.float32).astype(jnp.bfloat16)
    value_rows = jnp.dot(normed, value_part, preferred_element_type=jnp.float32).astype(jnp.bfloat16)
    per_group = HEADS // KV_HEADS
    query_heads = query_rows.astype(jnp.float32).reshape(seq_len, KV_HEADS, per_group, HEAD_DIM)
    key_heads = key_rows.astype(jnp.float32).reshape(seq_len, KV_HEADS, HEAD_DIM)
    value_heads = value_rows.astype(jnp.float32).reshape(seq_len, KV_HEADS, HEAD_DIM)
    scores = jnp.einsum('tgjd,sgd->gjts', query_heads, key_heads) / math.sqrt(HEAD_DIM)
    positions = jnp.arange(seq_len, dtype=jnp.int32)
    scores = jnp.where(positions[:, None] >= positions[None, :], scores, -1e+30)
    softmax_weights = jax.nn.softmax(scores, axis=-1).astype(jnp.bfloat16)
    heads_out = jnp.einsum('gjts,sgd->tgjd', softmax_weights.astype(jnp.float32), value_heads)
    heads_out = heads_out.astype(jnp.bfloat16).reshape(seq_len, HEADS * HEAD_DIM)
    grouped = heads_out.astype(jnp.float32).reshape(seq_len, N_TENSOR, -1)
    grouped_weight = output_part.astype(jnp.float32).reshape(N_TENSOR, -1, D)
    partials = jnp.einsum('tnc,ncd->ntd', grouped, grouped_weight)
    partials = lax.optimization_barrier(partials.astype(jnp.bfloat16)).astype(jnp.float32)
    attention_sum = lax.optimization_barrier(jnp.sum(partials, axis=0))
    return (token_rows.astype(jnp.float32) + attention_sum).astype(jnp.bfloat16)

def reference(section_input, history, query_weight, key_weight, value_weight, output_weight, mix_weights):
    block_outs = lax.map(one_section, (section_input, query_weight, key_weight, value_weight, output_weight))
    section_numbers = jnp.arange(N_SECTION, dtype=jnp.int32)
    mixed_sum = mix_weights[:, 0][:, None, None] * block_outs.astype(jnp.float32)
    for history_slot in range(1, HIST + 1):
        sender_section = section_numbers - DILATION_STRIDE * history_slot
        picked = jnp.take(history[:, history_slot - 1], jnp.maximum(sender_section, 0).astype(jnp.int32), axis=0)
        factor = jnp.where(sender_section >= 0, mix_weights[:, history_slot], jnp.float32(0.0))
        mixed_sum = mixed_sum + factor[:, None, None] * picked.astype(jnp.float32)
    mixed = mixed_sum.astype(jnp.bfloat16)
    return jnp.concatenate([mixed[-1:], mixed[:-1]], axis=0)
```

```python
import math

import jax
import jax.numpy as jnp
from jax import lax
from jax.sharding import PartitionSpec as P

HEAD_DIM = 64
DILATION_STRIDE = 4
COLUMN_PIECES = 4


def around(value, steps):
    count = lax.axis_size("tensor")
    return lax.ppermute(value, "tensor", [(i, (i + steps) % count) for i in range(count)])


def passed_along(value, steps):
    count = lax.axis_size("section")
    return lax.ppermute(value, "section", [(i, i + steps) for i in range(count - steps)])


def to_next_section(block):
    count = lax.axis_size("section")
    return lax.ppermute(block, "section", [(i, (i + 1) % count) for i in range(count)])


def normalize(token_rows):
    values = token_rows.astype(jnp.float32)
    inv_scale = lax.rsqrt(jnp.mean(values * values, axis=-1, keepdims=True) + 1e-05)
    return (values * inv_scale).astype(jnp.bfloat16)


def table_row(table, wanted):
    one_hot = (jnp.arange(table.shape[0], dtype=jnp.int32) == wanted).astype(jnp.float32)
    return jnp.sum(one_hot[:, None] * table, axis=0)


def rounded_dot(rows, weight):
    return jnp.dot(rows, weight, preferred_element_type=jnp.float32).astype(jnp.bfloat16)


def attend(query, key_rows, value_rows, row_positions, key_positions):
    rows, groups = query.shape[0], key_rows.shape[1]
    query_rows = query.reshape(rows, groups, -1, HEAD_DIM)
    scores = jnp.einsum(
        "tgjd,sgd->gjts", query_rows, key_rows, preferred_element_type=jnp.float32
    ) / math.sqrt(HEAD_DIM)
    scores = jnp.where(row_positions[:, None] >= key_positions[None, :], scores, -1e30)
    weights = jax.nn.softmax(scores, axis=-1).astype(jnp.bfloat16)
    heads_out = jnp.einsum("gjts,sgd->tgjd", weights, value_rows, preferred_element_type=jnp.float32)
    return heads_out.astype(jnp.bfloat16).reshape(rows, -1)


def on_device(
    section_input, history, query_weight, key_weight, value_weight, output_weight, mix_weights
):
    f32, bf16 = jnp.float32, jnp.bfloat16
    token_rows = section_input[0]
    rows, width = token_rows.shape
    half = rows // 2
    section, place = lax.axis_index("section"), lax.axis_index("tensor")
    ring = lax.axis_size("tensor")
    coefficient = table_row(mix_weights, section)
    wq, wk, wv, wo = query_weight[0], key_weight[0], value_weight[0], output_weight[0]

    normed = normalize(token_rows)
    top, bottom = normed[:half], normed[half:]
    left_top, right_bottom = around(top, 1), around(bottom, -1)
    left_bottom, right_top = around(bottom, 1), around(top, -1)
    opposite_top, opposite_bottom = around(left_top, 1), around(right_bottom, -1)

    slots = history.shape[1]
    received = [passed_along(history[0, k - 1], DILATION_STRIDE * k) for k in range(1, slots + 1)]

    def project(block):
        return rounded_dot(block, wq), rounded_dot(block, wk), rounded_dot(block, wv)

    q0, k0, v0 = project(normed)
    q1, k1, v1 = project(jnp.concatenate([left_top, left_bottom, right_top, right_bottom]))
    q3, k3, v3 = project(jnp.concatenate([opposite_top, opposite_bottom]))
    keys = jnp.concatenate([k0, k1, k3]).reshape(ring * rows, -1, HEAD_DIM)
    values = jnp.concatenate([v0, v1, v3]).reshape(ring * rows, -1, HEAD_DIM)
    blocks = jnp.stack([place, (place + ring - 1) % ring, (place + 1) % ring, (place + 2) % ring])
    positions = (blocks[:, None] * rows + jnp.arange(rows, dtype=jnp.int32)[None, :]).reshape(-1)

    out3 = rounded_dot(attend(q3, keys, values, positions[3 * rows :], positions), wo)
    from_left_merge = around(out3[:half], 1)
    from_right_merge = around(out3[half:], -1)
    out1 = rounded_dot(attend(q1, keys, values, positions[rows : 3 * rows], positions), wo)
    plain_left = around(out1[3 * half :], 1)
    plain_right = around(out1[:half], -1)
    out0 = rounded_dot(attend(q0, keys, values, positions[:rows], positions), wo)

    step = width // COLUMN_PIECES
    pieces = []
    for c in range(COLUMN_PIECES):
        cols = slice(c * step, (c + 1) * step)
        to_right = (out1[2 * half : 3 * half, cols].astype(f32) + from_left_merge[:, cols].astype(f32)).astype(bf16)
        to_left = (out1[half : 2 * half, cols].astype(f32) + from_right_merge[:, cols].astype(f32)).astype(bf16)
        merged_left = around(to_right, 1)
        merged_right = around(to_left, -1)
        from_left = jnp.concatenate([merged_left, plain_left[:, cols]]).astype(f32)
        from_right = jnp.concatenate([plain_right[:, cols], merged_right]).astype(f32)
        attention_sum = out0[:, cols].astype(f32) + from_left + from_right
        block_out = (token_rows[:, cols].astype(f32) + attention_sum).astype(bf16)
        mixed = coefficient[0] * block_out.astype(f32)
        for k in range(1, slots + 1):
            factor = jnp.where(section >= DILATION_STRIDE * k, coefficient[k], f32(0.0))
            mixed = mixed + factor * received[k - 1][:, cols].astype(f32)
        pieces.append(to_next_section(mixed.astype(bf16)))
    return jnp.concatenate(pieces, axis=1)[None]


def solution(mesh):
    placed = (
        P("section", "tensor", None),
        P("section", None, "tensor", None),
        P("section", None, "tensor"),
        P("section", None, "tensor"),
        P("section", None, "tensor"),
        P("section", "tensor", None),
        P(),
    )
    return jax.shard_map(
        on_device,
        mesh=mesh,
        in_specs=placed,
        out_specs=P("section", "tensor", None),
        check_vma=False,
    )
```

```python
import jax
import jax.numpy as jnp
from jax import lax
from jax.experimental import pallas as pl
from jax.experimental.pallas import tpu as pltpu
from jax.sharding import PartitionSpec as P


HEAD_DIM = 64
LANES = 128
LOG2_E = 1.4426950408889634
DILATION_STRIDE = 4
ROW = 2 * DILATION_STRIDE
COLUMN_PIECES = 2
PROJECTED_COLUMNS = 1024
MIB = 1 << 20
BF16, F32 = jnp.bfloat16, jnp.float32
BLOCK_OFFSETS = (0, 3, 1, 2)


def around(value, steps):
    count = lax.axis_size("tensor")
    return lax.ppermute(value, "tensor", [(i, (i + steps) % count) for i in range(count)])


def sent(value, sources, steps):
    return lax.ppermute(value, "section", [(i, i + steps(i)) for i in sources])


def to_next_section(block):
    count = lax.axis_size("section")
    return lax.ppermute(block, "section", [(i, (i + 1) % count) for i in range(count)])


def on_chip(body, outs, *args, limit=20, scratch=(), spaces=None):
    spaces = [pltpu.VMEM] * len(args) if spaces is None else spaces
    args = [
        value if space == pltpu.SMEM else pltpu.with_memory_space_constraint(value, space)
        for value, space in zip(args, spaces)
    ]
    return pl.pallas_call(
        body,
        out_shape=[pltpu.VMEM(shape, dtype) for shape, dtype in outs],
        in_specs=[pl.BlockSpec(memory_space=space) for space in spaces],
        out_specs=[pl.BlockSpec(memory_space=pltpu.VMEM)] * len(outs),
        scratch_shapes=list(scratch),
        compiler_params=pltpu.CompilerParams(vmem_limit_bytes=limit * MIB),
    )(*args)


def normalize_kernel(rows_ref, out):
    for start in range(0, out.shape[0], 16):
        rows = slice(start, start + 16)
        values = rows_ref[rows, :].astype(F32)
        inv_scale = lax.rsqrt(jnp.mean(values * values, axis=-1, keepdims=True) + 1e-05)
        out[rows, :] = (values * inv_scale).astype(BF16)


def load_kernel(wq, wk, wv, wo, inward, outward, sems):
    q, k = wq.shape[1], wk.shape[1]
    copies = [
        pltpu.make_async_copy(wq, inward.at[:, :q], sems.at[0]),
        pltpu.make_async_copy(wk, inward.at[:, q : q + k], sems.at[1]),
        pltpu.make_async_copy(wv, inward.at[:, q + k :], sems.at[2]),
        pltpu.make_async_copy(wo, outward, sems.at[3]),
    ]
    for copy in copies:
        copy.start()
    for copy in copies:
        copy.wait()


def place_in_grid():
    section = lax.axis_index("section")
    return section, section // ROW, section % ROW < DILATION_STRIDE


def coefficients(weights, section):
    at = lax.broadcasted_iota(jnp.int32, weights.shape, 1) == section
    column = jnp.sum(jnp.where(at, weights[...], F32(0.0)), axis=1, keepdims=True)
    return lambda k: column[k : k + 1, :]


def kept(condition, value):
    return jnp.where(condition, value, jnp.zeros_like(value))


def slots_kernel(pick):
    def kernel(history, *refs):
        outs, sems = refs[:-1], refs[-1]
        copies = [
            pltpu.make_async_copy(history.at[slot - 1], out, sems.at[i])
            for i, (slot, out) in enumerate(zip(pick(), outs))
        ]
        for copy in copies:
            copy.start()
        for copy in copies:
            copy.wait()

    return kernel


def first_slots():
    _, row, low = place_in_grid()
    return jnp.where(row < 2, jnp.where(low, 5, 3), jnp.where(low, 3, 1)), jnp.where(low, 7, 5)


def later_slots():
    _, _, low = place_in_grid()
    return jnp.where(low, 3, 1), 6, 4, 2, 1


def weighted(out, *terms):
    for start in range(0, out.shape[0], 16):
        rows = slice(start, start + 16)
        total = None
        for factor, block in terms:
            term = block[rows, :].astype(F32)
            term = term if factor is None else factor * term
            total = term if total is None else total + term
        out[rows, :] = total.astype(out.dtype)


def two_rows_kernel(weights, straight, crossed, out):
    section, _, low = place_in_grid()
    factor = coefficients(weights, jnp.minimum(section + 2 * ROW, weights.shape[1] - 1))
    weighted(out, (factor(4), straight), (jnp.where(low, factor(3), factor(5)), crossed))


def one_row_kernel(weights, straight, crossed_early, crossed_late, carried, out):
    section, row, low = place_in_grid()
    factor = coefficients(weights, jnp.minimum(section + ROW, weights.shape[1] - 1))
    crossed = jnp.where(low, factor(1), factor(3))
    weighted(
        out,
        (factor(2), straight),
        (kept(row == 2, crossed), crossed_early),
        (kept(row < 2, crossed), crossed_late),
        (None, carried),
    )


def cross_last_kernel(weights, far, same_row, out):
    section, row, low = place_in_grid()
    target = jnp.where(low, section + DILATION_STRIDE, jnp.maximum(section - DILATION_STRIDE, 0))
    factor = coefficients(weights, target)
    weighted(
        out,
        (kept(row == 3, jnp.where(low, factor(7), factor(5))), far),
        (kept(low, factor(1)), same_row),
    )


def projected(rows, inward):
    out = jnp.dot(rows, inward, preferred_element_type=F32)
    q_width = inward.shape[1] - 2 * LANES
    query = out[:, :q_width].astype(BF16)
    low = lax.broadcasted_iota(jnp.int32, (1, LANES), 1) < HEAD_DIM
    parts = []
    for start in (q_width, q_width + LANES):
        pair = out[:, start : start + LANES]
        swapped = pltpu.roll(pair, HEAD_DIM, 1)
        zero = jnp.zeros_like(pair)
        parts += [
            jnp.where(low, pair, zero),
            jnp.where(low, zero, swapped),
            jnp.where(low, swapped, zero),
            jnp.where(low, zero, pair),
        ]
    return query, jnp.concatenate([part.astype(BF16) for part in parts], axis=1)


def project_kernel(*refs):
    *blocks, inward, query_ref, kv_ref = refs
    rows = jnp.concatenate([block[...] for block in blocks], axis=0)
    query_ref[...], kv_ref[...] = projected(rows, inward[...])


def attended(query, kv, block):
    rows, place, ring = query.shape[0], lax.axis_index("tensor"), len(BLOCK_OFFSETS)
    row = lax.broadcasted_iota(jnp.int32, (rows, 1), 0) + (place + block) % ring * rows
    lane = lax.broadcasted_iota(jnp.int32, (1, rows), 1)
    key = jnp.concatenate([lane + (place + b) % ring * rows for b in BLOCK_OFFSETS], axis=1)
    bias = jnp.where(row >= key, F32(0.0), F32(-1e30))
    low = lax.broadcasted_iota(jnp.int32, (kv.shape[0], LANES), 1) < HEAD_DIM
    ones = [jnp.where(side, F32(1.0), F32(0.0)).astype(BF16) for side in (low, ~low)]
    out = []
    pairs = query.shape[1] // LANES
    for group in range(2):
        keys, values = [], []
        for side in range(2):
            at = (2 * group + side) * LANES
            keys.append(kv[:, at : at + LANES])
            values.append(jnp.concatenate([kv[:, 4 * LANES + at : 5 * LANES + at], ones[side]], axis=1))
        values = jnp.concatenate(values, axis=0)
        for pair in range(group * pairs // 2, (group + 1) * pairs // 2):
            q_pair = query[:, pair * LANES : (pair + 1) * LANES]
            weights = []
            for side in range(2):
                scores = lax.dot_general(q_pair, keys[side], (((1,), (1,)), ((), ())), preferred_element_type=F32)
                scores = scores + bias
                highest = jnp.max(scores, axis=-1, keepdims=True)
                weights.append(jnp.exp2((scores - highest) * F32(HEAD_DIM**-0.5 * LOG2_E)).astype(BF16))
            summed = jnp.dot(jnp.concatenate(weights, axis=1), values, preferred_element_type=F32)
            out.append((summed[:, :LANES] * (1.0 / summed[:, LANES:])).astype(BF16))
    return jnp.concatenate(out, axis=1)


def put_projected(heads, outward, top_ref, bottom_ref):
    half, width = top_ref.shape
    step = PROJECTED_COLUMNS
    for start in range(0, width, step):
        part = jnp.dot(heads, outward[:, start : start + step], preferred_element_type=F32).astype(BF16)
        top_ref[:, start : start + step] = part[:half]
        bottom_ref[:, start : start + step] = part[half:]


def opposite_kernel(top, bottom, inward, kv0, kv1, outward, out_top, out_bottom, kv_ref):
    rows = jnp.concatenate([top[...], bottom[...]], axis=0)
    query, kv3 = projected(rows, inward[...])
    kv_ref[...] = kv3
    kv = jnp.concatenate([kv0[...], kv1[...], kv3], axis=0)
    put_projected(attended(query, kv, BLOCK_OFFSETS[3]), outward, out_top, out_bottom)


def sides_kernel(query, kv0, kv1, kv3, outward, left_top, left_bottom, right_top, right_bottom):
    kv = jnp.concatenate([kv0[...], kv1[...], kv3[...]], axis=0)
    rows = query.shape[0] // 2
    put_projected(attended(query[:rows, :], kv, BLOCK_OFFSETS[1]), outward, left_top, left_bottom)
    put_projected(attended(query[rows:, :], kv, BLOCK_OFFSETS[2]), outward, right_top, right_bottom)


def own_kernel(query, kv0, kv1, kv3, outward, top, bottom):
    kv = jnp.concatenate([kv0[...], kv1[...], kv3[...]], axis=0)
    put_projected(attended(query[...], kv, BLOCK_OFFSETS[0]), outward, top, bottom)


def merge_kernel(right_top, right_bottom, left_top, left_bottom, from_left, from_right, *outs):
    half, width = right_top.shape
    count = len(outs) // 2
    step = width // count
    for c in range(count):
        cols = slice(c * step, (c + 1) * step)
        to_right, to_left = outs[c], outs[count + c]
        to_right[:half, :] = (right_top[:, cols].astype(F32) + from_left[:, cols].astype(F32)).astype(BF16)
        to_right[half:, :] = right_bottom[:, cols]
        to_left[:half, :] = left_top[:, cols]
        to_left[half:, :] = (left_bottom[:, cols].astype(F32) + from_right[:, cols].astype(F32)).astype(BF16)


def finish(piece):
    def kernel(weights, tokens, top, bottom, from_left, from_right, arrived, straight, crossed, out):
        half, step = top.shape[0], out.shape[1]
        section, row, _ = place_in_grid()
        factor = coefficients(weights, section)
        first, far = factor(0), kept(row == 3, factor(6))
        cols = slice(piece * step, (piece + 1) * step)
        for own, base in ((top, 0), (bottom, half)):
            for start in range(0, half, 16):
                rows, here = slice(base + start, base + start + 16), slice(start, start + 16)
                attention_sum = (
                    own[here, cols].astype(F32) + from_left[rows, :].astype(F32) + from_right[rows, :].astype(F32)
                )
                block_out = (tokens[rows, cols].astype(F32) + attention_sum).astype(BF16)
                past = arrived[rows, cols].astype(F32) + crossed[rows, cols].astype(F32)
                past = past + far * straight[rows, cols].astype(F32)
                out[rows, :] = (first * block_out.astype(F32) + past).astype(BF16)

    return kernel


def on_device(
    section_input, history, query_weight, key_weight, value_weight, output_weight, mix_weights
):
    token_rows = section_input[0]
    rows, width = token_rows.shape
    half, step = rows // 2, width // COLUMN_PIECES
    wq, wk, wv, wo = query_weight[0], key_weight[0], value_weight[0], output_weight[0]
    q_width, inward_width = wq.shape[1], wq.shape[1] + 2 * wk.shape[1]
    table = mix_weights.T
    half_block, block, kv_width = ((half, width), BF16), ((rows, width), BF16), 8 * LANES
    rows_of = lambda first, last: range(first * ROW, last * ROW)
    swap = lambda i: DILATION_STRIDE if i % ROW < DILATION_STRIDE else -DILATION_STRIDE

    (normed,) = on_chip(normalize_kernel, [block], token_rows, limit=6)
    left, right = around(normed, 1), around(normed, -1)
    opposite_top, opposite_bottom = around(left[:half], 1), around(right[half:], -1)

    stored = []
    for pick, count in ((first_slots, 2), (later_slots, 5)):
        stored += on_chip(
            slots_kernel(pick), [block] * count, history[0],
            limit=6, scratch=[pltpu.SemaphoreType.DMA((count,))], spaces=[pltpu.HBM],
        )
    early, far, late, far_straight, two_straight, one_straight, same_row = stored
    crossed_early = sent(early, rows_of(0, 3), swap)
    far_odd = sent(far, rows_of(0, 1), lambda i: 3 * ROW)
    crossed_late = sent(late, rows_of(0, 2), swap)
    far_even = sent(far_straight, rows_of(0, 1), lambda i: 3 * ROW)

    def combine(kernel, *blocks):
        return on_chip(kernel, [block], table, *blocks, limit=6)[0]

    two_rows = combine(two_rows_kernel, two_straight, crossed_early)
    carried = sent(two_rows, rows_of(0, 2), lambda i: ROW)
    last = combine(cross_last_kernel, far_odd, same_row)
    crossed_last = sent(last, [i for i in rows_of(0, 4) if i >= 3 * ROW or swap(i) > 0], swap)
    one_row = combine(one_row_kernel, one_straight, crossed_early, crossed_late, carried)
    arrived = sent(one_row, rows_of(0, 3), lambda i: ROW)

    inward, outward = on_chip(
        load_kernel, [((width, inward_width), BF16), (wo.shape, BF16)],
        wq, wk, wv, wo,
        limit=1, scratch=[pltpu.SemaphoreType.DMA((4,))], spaces=[pltpu.HBM] * 4,
    )
    q0, kv0 = on_chip(
        project_kernel, [((rows, q_width), BF16), ((rows, kv_width), BF16)], normed, inward,
        limit=12,
    )
    q1, kv1 = on_chip(
        project_kernel, [((2 * rows, q_width), BF16), ((2 * rows, kv_width), BF16)],
        left, right, inward, limit=16,
    )
    out3_top, out3_bottom, kv3 = on_chip(
        opposite_kernel, [half_block, half_block, ((rows, kv_width), BF16)],
        opposite_top, opposite_bottom, inward, kv0, kv1, outward,
    )
    from_left_merge, from_right_merge = around(out3_top, 1), around(out3_bottom, -1)
    left_out_top, left_out_bottom, right_out_top, right_out_bottom = on_chip(
        sides_kernel, [half_block] * 4, q1, kv0, kv1, kv3, outward
    )
    own_top, own_bottom = on_chip(own_kernel, [half_block] * 2, q0, kv0, kv1, kv3, outward)
    merged = on_chip(
        merge_kernel, [((rows, step), BF16)] * (2 * COLUMN_PIECES),
        right_out_top, right_out_bottom, left_out_top, left_out_bottom, from_left_merge, from_right_merge, limit=8,
    )
    pieces = []
    for c in range(COLUMN_PIECES):
        from_left = around(merged[c], 1)
        from_right = around(merged[COLUMN_PIECES + c], -1)
        (mixed,) = on_chip(
            finish(c), [((rows, step), BF16)], table, token_rows, own_top, own_bottom,
            from_left, from_right, arrived, far_even, crossed_last,
            limit=8,
        )
        pieces.append(to_next_section(mixed))
    return jnp.concatenate(pieces, axis=1)[None]


def solution(mesh):
    placed = (
        P("section", "tensor", None),
        P("section", None, "tensor", None),
        P("section", None, "tensor"),
        P("section", None, "tensor"),
        P("section", None, "tensor"),
        P("section", "tensor", None),
        P(),
    )

    return jax.shard_map(
        on_device,
        mesh=mesh,
        in_specs=placed,
        out_specs=P("section", "tensor", None),
        check_vma=False,
    )
```

```python
import jax
import jax.numpy as jnp
from jax import lax
from jax.experimental import pallas as pl
from jax.experimental.pallas import tpu as pltpu
from jax.sharding import PartitionSpec as P


HEAD_DIM = 64
LANES = 128
LOG2_E = 1.4426950408889634
DILATION_STRIDE = 4
ROW = 2 * DILATION_STRIDE
SPLIT = 5 / 8
PROJECTED_COLUMNS = 1024
MIB = 1 << 20
BF16, F32 = jnp.bfloat16, jnp.float32
BLOCK_OFFSETS = (0, 3, 1, 2)


def around(value, steps):
    count = lax.axis_size("tensor")
    return lax.ppermute(value, "tensor", [(i, (i + steps) % count) for i in range(count)])


def sent(value, sources, steps):
    return lax.ppermute(value, "section", [(i, i + steps(i)) for i in sources])


def to_next_section(block):
    count = lax.axis_size("section")
    return lax.ppermute(block, "section", [(i, (i + 1) % count) for i in range(count)])


def on_chip(body, outs, *args, limit=20, scratch=(), spaces=None):
    spaces = [pltpu.VMEM] * len(args) if spaces is None else spaces
    args = [
        value if space == pltpu.SMEM else pltpu.with_memory_space_constraint(value, space)
        for value, space in zip(args, spaces)
    ]
    return pl.pallas_call(
        body,
        out_shape=[pltpu.VMEM(shape, dtype) for shape, dtype in outs],
        in_specs=[pl.BlockSpec(memory_space=space) for space in spaces],
        out_specs=[pl.BlockSpec(memory_space=pltpu.VMEM)] * len(outs),
        scratch_shapes=list(scratch),
        compiler_params=pltpu.CompilerParams(vmem_limit_bytes=limit * MIB),
    )(*args)


def prologue_kernel(tokens, history, out, early, far, rows_ref, sems):
    token_copy = pltpu.make_async_copy(tokens, rows_ref, sems.at[0])
    token_copy.start()
    copies = [
        pltpu.make_async_copy(history.at[slot - 1], block, sems.at[1 + i])
        for i, (slot, block) in enumerate(zip(first_slots(), (early, far)))
    ]
    for copy in copies:
        copy.start()
    token_copy.wait()
    for start in range(0, out.shape[0], 16):
        rows = slice(start, start + 16)
        values = rows_ref[rows, :].astype(F32)
        inv_scale = lax.rsqrt(jnp.mean(values * values, axis=-1, keepdims=True) + 1e-05)
        out[rows, :] = (values * inv_scale).astype(BF16)
    for copy in copies:
        copy.wait()


def load_kernel(wk, wv, joined, sems):
    copies = [
        pltpu.make_async_copy(wk, joined.at[:, :LANES], sems.at[0]),
        pltpu.make_async_copy(wv, joined.at[:, LANES:], sems.at[1]),
    ]
    for copy in copies:
        copy.start()
    for copy in copies:
        copy.wait()


def place_in_grid():
    section = lax.axis_index("section")
    return section, section // ROW, section % ROW < DILATION_STRIDE


def coefficients(weights, section):
    at = lax.broadcasted_iota(jnp.int32, weights.shape, 1) == section
    column = jnp.sum(jnp.where(at, weights[...], F32(0.0)), axis=1, keepdims=True)
    return lambda k: column[k : k + 1, :]


def kept(condition, value):
    return jnp.where(condition, value, jnp.zeros_like(value))


def slots_kernel(history, *refs):
    outs, sems = refs[:-1], refs[-1]
    _, _, low = place_in_grid()
    slots = (jnp.where(low, 3, 1), 6, 4, 2, 1)
    copies = [
        pltpu.make_async_copy(history.at[slot - 1], out, sems.at[i])
        for i, (slot, out) in enumerate(zip(slots, outs))
    ]
    for copy in copies:
        copy.start()
    for copy in copies:
        copy.wait()


def first_slots():
    _, row, low = place_in_grid()
    return jnp.where(row < 2, jnp.where(low, 5, 3), jnp.where(low, 3, 1)), jnp.where(low, 7, 5)


def weighted(out, first_column, *terms):
    width = out.shape[1]
    for start in range(0, out.shape[0], 16):
        rows = slice(start, start + 16)
        total = None
        for factor, block in terms:
            first = first_column if block.shape[1] > width else 0
            term = block[rows, first : first + width].astype(F32)
            term = term if factor is None else factor * term
            total = term if total is None else total + term
        out[rows, :] = total.astype(out.dtype)


def two_rows_kernel(weights, straight, crossed, *outs):
    section, _, low = place_in_grid()
    factor = coefficients(weights, jnp.minimum(section + 2 * ROW, weights.shape[1] - 1))
    first = 0
    for out in outs:
        weighted(out, first, (factor(4), straight), (jnp.where(low, factor(3), factor(5)), crossed))
        first += out.shape[1]


def one_row(first_column):
    def kernel(weights, straight, crossed_early, crossed_late, carried, out):
        section, row, low = place_in_grid()
        factor = coefficients(weights, jnp.minimum(section + ROW, weights.shape[1] - 1))
        crossed = jnp.where(low, factor(1), factor(3))
        weighted(
            out,
            first_column,
            (factor(2), straight),
            (kept(row == 2, crossed), crossed_early),
            (kept(row < 2, crossed), crossed_late),
            (None, carried),
        )

    return kernel


def projected(rows, wq, joined):
    query = jnp.dot(rows, wq, preferred_element_type=F32).astype(BF16)
    out = jnp.dot(rows, joined, preferred_element_type=F32)
    low = lax.broadcasted_iota(jnp.int32, (1, LANES), 1) < HEAD_DIM
    parts = []
    for start in (0, LANES):
        pair = out[:, start : start + LANES]
        swapped = pltpu.roll(pair, HEAD_DIM, 1)
        zero = jnp.zeros_like(pair)
        parts += [
            jnp.where(low, pair, zero),
            jnp.where(low, zero, swapped),
            jnp.where(low, swapped, zero),
            jnp.where(low, zero, pair),
        ]
    return query, jnp.concatenate([part.astype(BF16) for part in parts], axis=1)


def project_kernel(*refs):
    *blocks, wq, joined, query_ref, kv_ref = refs
    rows = jnp.concatenate([block[...] for block in blocks], axis=0)
    query_ref[...], kv_ref[...] = projected(rows, wq[...], joined[...])


def attended(query, kv, block):
    rows, place, ring = query.shape[0], lax.axis_index("tensor"), len(BLOCK_OFFSETS)
    row = lax.broadcasted_iota(jnp.int32, (rows, 1), 0) + (place + block) % ring * rows
    lane = lax.broadcasted_iota(jnp.int32, (1, rows), 1)
    key = jnp.concatenate([lane + (place + b) % ring * rows for b in BLOCK_OFFSETS], axis=1)
    bias = jnp.where(row >= key, F32(0.0), F32(-1e30))
    low = lax.broadcasted_iota(jnp.int32, (kv.shape[0], LANES), 1) < HEAD_DIM
    ones = [jnp.where(side, F32(1.0), F32(0.0)).astype(BF16) for side in (low, ~low)]
    out = []
    pairs = query.shape[1] // LANES
    for group in range(2):
        keys, values = [], []
        for side in range(2):
            at = (2 * group + side) * LANES
            keys.append(kv[:, at : at + LANES])
            values.append(jnp.concatenate([kv[:, 4 * LANES + at : 5 * LANES + at], ones[side]], axis=1))
        values = jnp.concatenate(values, axis=0)
        for pair in range(group * pairs // 2, (group + 1) * pairs // 2):
            q_pair = query[:, pair * LANES : (pair + 1) * LANES]
            weights = []
            for side in range(2):
                scores = lax.dot_general(q_pair, keys[side], (((1,), (1,)), ((), ())), preferred_element_type=F32)
                scores = scores + bias
                highest = jnp.max(scores, axis=-1, keepdims=True)
                weights.append(jnp.exp2((scores - highest) * F32(HEAD_DIM**-0.5 * LOG2_E)).astype(BF16))
            summed = jnp.dot(jnp.concatenate(weights, axis=1), values, preferred_element_type=F32)
            out.append((summed[:, :LANES] * (1.0 / summed[:, LANES:])).astype(BF16))
    return jnp.concatenate(out, axis=1)


def put_projected(heads, outward, top_ref, bottom_ref):
    half, width = top_ref.shape
    step = PROJECTED_COLUMNS
    for start in range(0, width, step):
        part = jnp.dot(heads, outward[:, start : start + step], preferred_element_type=F32).astype(BF16)
        top_ref[:, start : start + step] = part[:half]
        bottom_ref[:, start : start + step] = part[half:]


def opposite_kernel(top, bottom, wq, joined, kv0, kv1, outward, out_top, out_bottom, kv_ref):
    rows = jnp.concatenate([top[...], bottom[...]], axis=0)
    query, kv3 = projected(rows, wq[...], joined[...])
    kv_ref[...] = kv3
    kv = jnp.concatenate([kv0[...], kv1[...], kv3], axis=0)
    put_projected(attended(query, kv, BLOCK_OFFSETS[3]), outward, out_top, out_bottom)


def sides_kernel(query, kv0, kv1, kv3, outward, left_top, left_bottom, right_top, right_bottom):
    kv = jnp.concatenate([kv0[...], kv1[...], kv3[...]], axis=0)
    rows = query.shape[0] // 2
    put_projected(attended(query[:rows, :], kv, BLOCK_OFFSETS[1]), outward, left_top, left_bottom)
    put_projected(attended(query[rows:, :], kv, BLOCK_OFFSETS[2]), outward, right_top, right_bottom)


def own_kernel(query, kv0, kv1, kv3, outward, top, bottom):
    kv = jnp.concatenate([kv0[...], kv1[...], kv3[...]], axis=0)
    put_projected(attended(query[...], kv, BLOCK_OFFSETS[0]), outward, top, bottom)


def merge_kernel(right_top, right_bottom, left_top, left_bottom, from_left, from_right, *outs):
    half = right_top.shape[0]
    count, start = len(outs) // 2, 0
    for c in range(count):
        cols = slice(start, start + outs[c].shape[1])
        start = cols.stop
        to_right, to_left = outs[c], outs[count + c]
        to_right[:half, :] = (right_top[:, cols].astype(F32) + from_left[:, cols].astype(F32)).astype(BF16)
        to_right[half:, :] = right_bottom[:, cols]
        to_left[:half, :] = left_top[:, cols]
        to_left[half:, :] = (left_bottom[:, cols].astype(F32) + from_right[:, cols].astype(F32)).astype(BF16)


def finish(first_column):
    def kernel(weights, tokens, top, bottom, from_left, from_right, arrived, straight, crossed, same_row, out):
        half = top.shape[0]
        section, row, low = place_in_grid()
        factor = coefficients(weights, section)
        cols = slice(first_column, first_column + out.shape[1])
        far, far_odd = kept(row == 3, factor(6)), kept(row == 3, jnp.where(low, factor(5), factor(7)))
        near = kept(jnp.logical_not(low), factor(1))
        for own, base in ((top, 0), (bottom, half)):
            for start in range(0, half, 16):
                rows, here = slice(base + start, base + start + 16), slice(start, start + 16)
                attention_sum = (
                    own[here, cols].astype(F32) + from_left[rows, :].astype(F32) + from_right[rows, :].astype(F32)
                )
                block_out = (tokens[rows, cols].astype(F32) + attention_sum).astype(BF16)
                past = arrived[rows, :].astype(F32) + far * straight[rows, cols].astype(F32)
                past = past + far_odd * crossed[rows, cols].astype(F32)
                past = past + near * same_row[rows, cols].astype(F32)
                out[rows, :] = (factor(0) * block_out.astype(F32) + past).astype(BF16)

    return kernel


def on_device(
    section_input, history, query_weight, key_weight, value_weight, output_weight, mix_weights
):
    token_rows = section_input[0]
    rows, width = token_rows.shape
    half, sizes = rows // 2, (int(width * SPLIT), width - int(width * SPLIT))
    wq, wk, wv, wo = query_weight[0], key_weight[0], value_weight[0], output_weight[0]
    q_width = wq.shape[1]
    table = mix_weights.T
    half_block, block, kv_width = ((half, width), BF16), ((rows, width), BF16), 8 * LANES
    rows_of = lambda first, last: range(first * ROW, last * ROW)
    swap = lambda i: DILATION_STRIDE if i % ROW < DILATION_STRIDE else -DILATION_STRIDE

    normed, early, far = on_chip(
        prologue_kernel, [block] * 3, token_rows, history[0], limit=6,
        scratch=[pltpu.VMEM((rows, width), BF16), pltpu.SemaphoreType.DMA((3,))], spaces=[pltpu.HBM] * 2,
    )
    left, right = around(normed, 1), around(normed, -1)
    opposite_top, opposite_bottom = around(left[:half], 1), around(right[half:], -1)

    pieces_of = [((rows, size), BF16) for size in sizes]
    late, far_straight, two_straight, one_straight, same_row = on_chip(
        slots_kernel, [block] * 5, history[0],
        limit=6, scratch=[pltpu.SemaphoreType.DMA((5,))], spaces=[pltpu.HBM],
    )
    crossed_early = sent(early, rows_of(0, 3), swap)
    far_odd = sent(far, rows_of(0, 1), lambda i: 3 * ROW + swap(i))
    crossed_late = sent(late, rows_of(0, 2), swap)
    far_even = sent(far_straight, rows_of(0, 1), lambda i: 3 * ROW)

    two_rows = on_chip(two_rows_kernel, pieces_of, table, two_straight, crossed_early, limit=6)
    carried = [sent(piece, rows_of(0, 2), lambda i: ROW) for piece in two_rows]
    near_row = sent(same_row, [i for i in rows_of(0, 4) if swap(i) > 0], swap)
    arrived = []
    for c, piece in enumerate(pieces_of):
        (summed,) = on_chip(
            one_row(sum(sizes[:c])), [piece],
            table, one_straight, crossed_early, crossed_late, carried[c], limit=6,
        )
        arrived.append(sent(summed, rows_of(0, 3), lambda i: ROW))

    (joined,) = on_chip(
        load_kernel, [((width, 2 * LANES), BF16)], wk, wv,
        limit=3, scratch=[pltpu.SemaphoreType.DMA((2,))], spaces=[pltpu.HBM] * 2,
    )
    q0, kv0 = on_chip(
        project_kernel, [((rows, q_width), BF16), ((rows, kv_width), BF16)], normed, wq, joined,
        limit=12,
    )
    q1, kv1 = on_chip(
        project_kernel, [((2 * rows, q_width), BF16), ((2 * rows, kv_width), BF16)],
        left, right, wq, joined, limit=16,
    )
    out3_top, out3_bottom, kv3 = on_chip(
        opposite_kernel, [half_block, half_block, ((rows, kv_width), BF16)],
        opposite_top, opposite_bottom, wq, joined, kv0, kv1, wo,
    )
    from_left_merge, from_right_merge = around(out3_top, 1), around(out3_bottom, -1)
    left_out_top, left_out_bottom, right_out_top, right_out_bottom = on_chip(
        sides_kernel, [half_block] * 4, q1, kv0, kv1, kv3, wo
    )
    own_top, own_bottom = on_chip(own_kernel, [half_block] * 2, q0, kv0, kv1, kv3, wo)
    merged = on_chip(
        merge_kernel, [((rows, size), BF16) for size in 2 * sizes],
        right_out_top, right_out_bottom, left_out_top, left_out_bottom, from_left_merge, from_right_merge, limit=8,
    )
    pieces = []
    for c, size in enumerate(sizes):
        from_left = around(merged[c], 1)
        from_right = around(merged[len(sizes) + c], -1)
        (mixed,) = on_chip(
            finish(sum(sizes[:c])), [((rows, size), BF16)], table, token_rows, own_top, own_bottom,
            from_left, from_right, arrived[c], far_even, far_odd, near_row, limit=8,
        )
        pieces.append(to_next_section(mixed))
    return jnp.concatenate(pieces, axis=1)[None]


def solution(mesh):
    placed = (
        P("section", "tensor", None),
        P("section", None, "tensor", None),
        P("section", None, "tensor"),
        P("section", None, "tensor"),
        P("section", None, "tensor"),
        P("section", "tensor", None),
        P(),
    )

    return jax.shard_map(
        on_device,
        mesh=mesh,
        in_specs=placed,
        out_specs=P("section", "tensor", None),
        check_vma=False,
    )
```

```python
import jax
import jax.numpy as jnp
from jax import lax
from jax.experimental import pallas as pl
from jax.experimental.pallas import tpu as pltpu
from jax.sharding import PartitionSpec as P


HEAD_DIM = 64
LANES = 128
LOG2_E = 1.4426950408889634
DILATION_STRIDE = 4
ROW = 2 * DILATION_STRIDE
CARRIED_PIECES = (5, 3)
MERGED_PIECES = (5, 5, 6)
PROJECTED_COLUMNS = 1024
MIB = 1 << 20
BF16, F32 = jnp.bfloat16, jnp.float32
BLOCK_OFFSETS = (0, 3, 1, 2)


def around(value, steps):
    count = lax.axis_size("tensor")
    return lax.ppermute(value, "tensor", [(i, (i + steps) % count) for i in range(count)])


def sent(value, sources, steps):
    return lax.ppermute(value, "section", [(i, i + steps(i)) for i in sources])


def to_next_section(block):
    count = lax.axis_size("section")
    return lax.ppermute(block, "section", [(i, (i + 1) % count) for i in range(count)])


def on_chip(body, outs, *args, limit=20, scratch=(), spaces=None):
    spaces = [pltpu.VMEM] * len(args) if spaces is None else spaces
    args = [
        value if space == pltpu.SMEM else pltpu.with_memory_space_constraint(value, space)
        for value, space in zip(args, spaces)
    ]
    return pl.pallas_call(
        body,
        out_shape=[pltpu.VMEM(shape, dtype) for shape, dtype in outs],
        in_specs=[pl.BlockSpec(memory_space=space) for space in spaces],
        out_specs=[pl.BlockSpec(memory_space=pltpu.VMEM)] * len(outs),
        scratch_shapes=list(scratch),
        compiler_params=pltpu.CompilerParams(vmem_limit_bytes=limit * MIB),
    )(*args)


def prologue_kernel(tokens, history, out, early, far, rows_ref, sems):
    token_copy = pltpu.make_async_copy(tokens, rows_ref, sems.at[0])
    token_copy.start()
    copies = [
        pltpu.make_async_copy(history.at[slot - 1], block, sems.at[1 + i])
        for i, (slot, block) in enumerate(zip(first_slots(), (early, far)))
    ]
    for copy in copies:
        copy.start()
    token_copy.wait()
    for start in range(0, out.shape[0], 16):
        rows = slice(start, start + 16)
        values = rows_ref[rows, :].astype(F32)
        inv_scale = lax.rsqrt(jnp.mean(values * values, axis=-1, keepdims=True) + 1e-05)
        out[rows, :] = (values * inv_scale).astype(BF16)
    for copy in copies:
        copy.wait()


def load_kernel(wk, wv, joined, sems):
    copies = [
        pltpu.make_async_copy(wk, joined.at[:, :LANES], sems.at[0]),
        pltpu.make_async_copy(wv, joined.at[:, LANES:], sems.at[1]),
    ]
    for copy in copies:
        copy.start()
    for copy in copies:
        copy.wait()


def place_in_grid():
    section = lax.axis_index("section")
    return section, section // ROW, section % ROW < DILATION_STRIDE


def coefficients(weights, section):
    at = lax.broadcasted_iota(jnp.int32, weights.shape, 1) == section
    column = jnp.sum(jnp.where(at, weights[...], F32(0.0)), axis=1, keepdims=True)
    return lambda k: column[k : k + 1, :]


def kept(condition, value):
    return jnp.where(condition, value, jnp.zeros_like(value))


def slots_kernel(history, *refs):
    outs, sems = refs[:-1], refs[-1]
    _, _, low = place_in_grid()
    slots = (jnp.where(low, 3, 1), 6, 4, 2, 1)
    copies = [
        pltpu.make_async_copy(history.at[slot - 1], out, sems.at[i])
        for i, (slot, out) in enumerate(zip(slots, outs))
    ]
    for copy in copies:
        copy.start()
    for copy in copies:
        copy.wait()


def first_slots():
    _, row, low = place_in_grid()
    return jnp.where(row < 2, jnp.where(low, 5, 3), jnp.where(low, 3, 1)), jnp.where(low, 7, 5)


def weighted(out, first_column, *terms):
    width = out.shape[1]
    for start in range(0, out.shape[0], 16):
        rows = slice(start, start + 16)
        total = None
        for factor, block in terms:
            first = first_column if block.shape[1] > width else 0
            term = block[rows, first : first + width].astype(F32)
            term = term if factor is None else factor * term
            total = term if total is None else total + term
        out[rows, :] = total.astype(out.dtype)


def two_rows_kernel(weights, straight, crossed, *outs):
    section, _, low = place_in_grid()
    factor = coefficients(weights, jnp.minimum(section + 2 * ROW, weights.shape[1] - 1))
    first = 0
    for out in outs:
        weighted(out, first, (factor(4), straight), (jnp.where(low, factor(3), factor(5)), crossed))
        first += out.shape[1]


def one_row(first_column):
    def kernel(weights, straight, crossed_early, crossed_late, carried, out):
        section, row, low = place_in_grid()
        factor = coefficients(weights, jnp.minimum(section + ROW, weights.shape[1] - 1))
        crossed = jnp.where(low, factor(1), factor(3))
        weighted(
            out,
            first_column,
            (factor(2), straight),
            (kept(row == 2, crossed), crossed_early),
            (kept(row < 2, crossed), crossed_late),
            (None, carried),
        )

    return kernel


def projected(rows, wq, joined):
    query = jnp.dot(rows, wq, preferred_element_type=F32).astype(BF16)
    out = jnp.dot(rows, joined, preferred_element_type=F32)
    low = lax.broadcasted_iota(jnp.int32, (1, LANES), 1) < HEAD_DIM
    parts = []
    for start in (0, LANES):
        pair = out[:, start : start + LANES]
        swapped = pltpu.roll(pair, HEAD_DIM, 1)
        zero = jnp.zeros_like(pair)
        parts += [
            jnp.where(low, pair, zero),
            jnp.where(low, zero, swapped),
            jnp.where(low, swapped, zero),
            jnp.where(low, zero, pair),
        ]
    return query, jnp.concatenate([part.astype(BF16) for part in parts], axis=1)


def project_kernel(*refs):
    *blocks, wq, joined, query_ref, kv_ref = refs
    rows = jnp.concatenate([block[...] for block in blocks], axis=0)
    query_ref[...], kv_ref[...] = projected(rows, wq[...], joined[...])


def attended(query, kv, block):
    rows, place, ring = query.shape[0], lax.axis_index("tensor"), len(BLOCK_OFFSETS)
    row = lax.broadcasted_iota(jnp.int32, (rows, 1), 0) + (place + block) % ring * rows
    lane = lax.broadcasted_iota(jnp.int32, (1, rows), 1)
    key = jnp.concatenate([lane + (place + b) % ring * rows for b in BLOCK_OFFSETS], axis=1)
    bias = jnp.where(row >= key, F32(0.0), F32(-1e30))
    low = lax.broadcasted_iota(jnp.int32, (kv.shape[0], LANES), 1) < HEAD_DIM
    ones = [jnp.where(side, F32(1.0), F32(0.0)).astype(BF16) for side in (low, ~low)]
    out = []
    pairs = query.shape[1] // LANES
    for group in range(2):
        keys, values = [], []
        for side in range(2):
            at = (2 * group + side) * LANES
            keys.append(kv[:, at : at + LANES])
            values.append(jnp.concatenate([kv[:, 4 * LANES + at : 5 * LANES + at], ones[side]], axis=1))
        values = jnp.concatenate(values, axis=0)
        for pair in range(group * pairs // 2, (group + 1) * pairs // 2):
            q_pair = query[:, pair * LANES : (pair + 1) * LANES]
            weights = []
            for side in range(2):
                scores = lax.dot_general(q_pair, keys[side], (((1,), (1,)), ((), ())), preferred_element_type=F32)
                scores = scores + bias
                highest = jnp.max(scores, axis=-1, keepdims=True)
                weights.append(jnp.exp2((scores - highest) * F32(HEAD_DIM**-0.5 * LOG2_E)).astype(BF16))
            summed = jnp.dot(jnp.concatenate(weights, axis=1), values, preferred_element_type=F32)
            out.append((summed[:, :LANES] * (1.0 / summed[:, LANES:])).astype(BF16))
    return jnp.concatenate(out, axis=1)


def put_projected(heads, outward, top_ref, bottom_ref):
    half, width = top_ref.shape
    step = PROJECTED_COLUMNS
    for start in range(0, width, step):
        part = jnp.dot(heads, outward[:, start : start + step], preferred_element_type=F32).astype(BF16)
        top_ref[:, start : start + step] = part[:half]
        bottom_ref[:, start : start + step] = part[half:]


def opposite_kernel(top, bottom, wq, joined, kv0, kv1, outward, out_top, out_bottom, kv_ref):
    rows = jnp.concatenate([top[...], bottom[...]], axis=0)
    query, kv3 = projected(rows, wq[...], joined[...])
    kv_ref[...] = kv3
    kv = jnp.concatenate([kv0[...], kv1[...], kv3], axis=0)
    put_projected(attended(query, kv, BLOCK_OFFSETS[3]), outward, out_top, out_bottom)


def sides_kernel(query, kv0, kv1, kv3, outward, left_top, left_bottom, right_top, right_bottom):
    kv = jnp.concatenate([kv0[...], kv1[...], kv3[...]], axis=0)
    rows = query.shape[0] // 2
    put_projected(attended(query[:rows, :], kv, BLOCK_OFFSETS[1]), outward, left_top, left_bottom)
    put_projected(attended(query[rows:, :], kv, BLOCK_OFFSETS[2]), outward, right_top, right_bottom)


def own_kernel(query, kv0, kv1, kv3, outward, top, bottom):
    kv = jnp.concatenate([kv0[...], kv1[...], kv3[...]], axis=0)
    put_projected(attended(query[...], kv, BLOCK_OFFSETS[0]), outward, top, bottom)


def merge_kernel(right_top, left_bottom, from_left, from_right, *outs):
    count, start = len(outs) // 2, 0
    for c in range(count):
        cols = slice(start, start + outs[c].shape[1])
        start = cols.stop
        outs[c][...] = (right_top[:, cols].astype(F32) + from_left[:, cols].astype(F32)).astype(BF16)
        outs[count + c][...] = (left_bottom[:, cols].astype(F32) + from_right[:, cols].astype(F32)).astype(BF16)


def finish(first_column, first_arrived):
    def kernel(weights, tokens, *refs):
        *parts, arrived, straight, crossed, same_row, out = refs
        half = out.shape[0] // 2
        section, row, low = place_in_grid()
        factor = coefficients(weights, section)
        cols = slice(first_column, first_column + out.shape[1])
        there = slice(first_arrived, first_arrived + out.shape[1])
        far, far_odd = kept(row == 3, factor(6)), kept(row == 3, jnp.where(low, factor(5), factor(7)))
        near = kept(jnp.logical_not(low), factor(1))
        for base, (own, plain, merged) in ((0, parts[:3]), (half, parts[3:])):
            for start in range(0, half, 16):
                rows, here = slice(base + start, base + start + 16), slice(start, start + 16)
                attention_sum = own[here, cols].astype(F32) + plain[here, cols].astype(F32)
                attention_sum = attention_sum + merged[here, :].astype(F32)
                block_out = (tokens[rows, cols].astype(F32) + attention_sum).astype(BF16)
                past = arrived[rows, there].astype(F32) + far * straight[rows, cols].astype(F32)
                past = past + far_odd * crossed[rows, cols].astype(F32)
                past = past + near * same_row[rows, cols].astype(F32)
                out[rows, :] = (factor(0) * block_out.astype(F32) + past).astype(BF16)

    return kernel


def cut(width, proportions):
    return [width * part // sum(proportions) for part in proportions]


def on_device(
    section_input, history, query_weight, key_weight, value_weight, output_weight, mix_weights
):
    token_rows = section_input[0]
    rows, width = token_rows.shape
    half, sizes = rows // 2, cut(width, CARRIED_PIECES)
    wq, wk, wv, wo = query_weight[0], key_weight[0], value_weight[0], output_weight[0]
    q_width = wq.shape[1]
    table = mix_weights.T
    half_block, block, kv_width = ((half, width), BF16), ((rows, width), BF16), 8 * LANES
    rows_of = lambda first, last: range(first * ROW, last * ROW)
    swap = lambda i: DILATION_STRIDE if i % ROW < DILATION_STRIDE else -DILATION_STRIDE

    normed, early, far = on_chip(
        prologue_kernel, [block] * 3, token_rows, history[0], limit=6,
        scratch=[pltpu.VMEM((rows, width), BF16), pltpu.SemaphoreType.DMA((3,))], spaces=[pltpu.HBM] * 2,
    )
    left, right = around(normed, 1), around(normed, -1)
    opposite_top, opposite_bottom = around(left[:half], 1), around(right[half:], -1)

    pieces_of = [((rows, size), BF16) for size in sizes]
    late, far_straight, two_straight, one_straight, same_row = on_chip(
        slots_kernel, [block] * 5, history[0],
        limit=6, scratch=[pltpu.SemaphoreType.DMA((5,))], spaces=[pltpu.HBM],
    )
    crossed_early = sent(early, rows_of(0, 3), swap)
    far_odd = sent(far, rows_of(0, 1), lambda i: 3 * ROW + swap(i))
    crossed_late = sent(late, rows_of(0, 2), swap)
    far_even = sent(far_straight, rows_of(0, 1), lambda i: 3 * ROW)

    two_rows = on_chip(two_rows_kernel, pieces_of, table, two_straight, crossed_early, limit=6)
    carried = [sent(piece, rows_of(0, 2), lambda i: ROW) for piece in two_rows]
    near_row = sent(same_row, [i for i in rows_of(0, 4) if swap(i) > 0], swap)
    arrived = []
    for c, piece in enumerate(pieces_of):
        (summed,) = on_chip(
            one_row(sum(sizes[:c])), [piece],
            table, one_straight, crossed_early, crossed_late, carried[c], limit=6,
        )
        arrived.append(sent(summed, rows_of(0, 3), lambda i: ROW))

    (joined,) = on_chip(
        load_kernel, [((width, 2 * LANES), BF16)], wk, wv,
        limit=3, scratch=[pltpu.SemaphoreType.DMA((2,))], spaces=[pltpu.HBM] * 2,
    )
    q0, kv0 = on_chip(
        project_kernel, [((rows, q_width), BF16), ((rows, kv_width), BF16)], normed, wq, joined,
        limit=12,
    )
    q1, kv1 = on_chip(
        project_kernel, [((2 * rows, q_width), BF16), ((2 * rows, kv_width), BF16)],
        left, right, wq, joined, limit=16,
    )
    out3_top, out3_bottom, kv3 = on_chip(
        opposite_kernel, [half_block, half_block, ((rows, kv_width), BF16)],
        opposite_top, opposite_bottom, wq, joined, kv0, kv1, wo,
    )
    from_left_merge, from_right_merge = around(out3_top, 1), around(out3_bottom, -1)
    left_out_top, left_out_bottom, right_out_top, right_out_bottom = on_chip(
        sides_kernel, [half_block] * 4, q1, kv0, kv1, kv3, wo
    )
    plain_left, plain_right = around(right_out_bottom, 1), around(left_out_top, -1)
    own_top, own_bottom = on_chip(own_kernel, [half_block] * 2, q0, kv0, kv1, kv3, wo)
    merged_sizes, pieces, first = cut(width, MERGED_PIECES), [], 0
    merged = on_chip(
        merge_kernel, [((half, size), BF16) for size in 2 * merged_sizes],
        right_out_top, left_out_bottom, from_left_merge, from_right_merge, limit=8,
    )
    for c, size in enumerate(merged_sizes):
        merged_left = around(merged[c], 1)
        merged_right = around(merged[len(merged_sizes) + c], -1)
        piece = 0 if first + size <= sizes[0] else 1
        (mixed,) = on_chip(
            finish(first, first - sizes[0] * piece), [((rows, size), BF16)], table, token_rows,
            own_top, plain_right, merged_left, own_bottom, plain_left, merged_right,
            arrived[piece], far_even, far_odd, near_row, limit=8,
        )
        pieces.append(to_next_section(mixed))
        first += size
    return jnp.concatenate(pieces, axis=1)[None]


def solution(mesh):
    placed = (
        P("section", "tensor", None),
        P("section", None, "tensor", None),
        P("section", None, "tensor"),
        P("section", None, "tensor"),
        P("section", None, "tensor"),
        P("section", "tensor", None),
        P(),
    )

    return jax.shard_map(
        on_device,
        mesh=mesh,
        in_specs=placed,
        out_specs=P("section", "tensor", None),
        check_vma=False,
    )
```

```python
import jax
import jax.numpy as jnp
from jax import lax
from jax.experimental import pallas as pl
from jax.experimental.pallas import tpu as pltpu
from jax.sharding import PartitionSpec as P


HEAD_DIM = 64
LANES = 128
LOG2_E = 1.4426950408889634
DILATION_STRIDE = 4
ROW = 2 * DILATION_STRIDE
CARRIED_PIECES = (5, 3)
MERGED_PIECES = (5, 5, 6)
PROJECTED_COLUMNS = 1024
MIB = 1 << 20
BF16, F32 = jnp.bfloat16, jnp.float32
BLOCK_OFFSETS = (0, 3, 1, 2)


def around(value, steps):
    count = lax.axis_size("tensor")
    return lax.ppermute(value, "tensor", [(i, (i + steps) % count) for i in range(count)])


def sent(value, sources, steps):
    return lax.ppermute(value, "section", [(i, i + steps(i)) for i in sources])


def to_next_section(block):
    count = lax.axis_size("section")
    return lax.ppermute(block, "section", [(i, (i + 1) % count) for i in range(count)])


def on_chip(body, outs, *args, limit=20, scratch=(), spaces=None):
    spaces = [pltpu.VMEM] * len(args) if spaces is None else spaces
    args = [
        value if space == pltpu.SMEM else pltpu.with_memory_space_constraint(value, space)
        for value, space in zip(args, spaces)
    ]
    return pl.pallas_call(
        body,
        out_shape=[pltpu.VMEM(shape, dtype) for shape, dtype in outs],
        in_specs=[pl.BlockSpec(memory_space=space) for space in spaces],
        out_specs=[pl.BlockSpec(memory_space=pltpu.VMEM)] * len(outs),
        scratch_shapes=list(scratch),
        compiler_params=pltpu.CompilerParams(vmem_limit_bytes=limit * MIB),
    )(*args)


def prologue_kernel(tokens, history, out, early, rows_ref, sems):
    token_copy = pltpu.make_async_copy(tokens, rows_ref, sems.at[0])
    token_copy.start()
    copies = [
        pltpu.make_async_copy(history.at[slot - 1], block, sems.at[1 + i])
        for i, (slot, block) in enumerate(zip(first_slots()[:1], (early,)))
    ]
    for copy in copies:
        copy.start()
    token_copy.wait()
    for start in range(0, out.shape[0], 16):
        rows = slice(start, start + 16)
        values = rows_ref[rows, :].astype(F32)
        inv_scale = lax.rsqrt(jnp.mean(values * values, axis=-1, keepdims=True) + 1e-05)
        out[rows, :] = (values * inv_scale).astype(BF16)
    for copy in copies:
        copy.wait()


def load_kernel(wk, wv, joined, sems):
    copies = [
        pltpu.make_async_copy(wk, joined.at[:, :LANES], sems.at[0]),
        pltpu.make_async_copy(wv, joined.at[:, LANES:], sems.at[1]),
    ]
    for copy in copies:
        copy.start()
    for copy in copies:
        copy.wait()


def place_in_grid():
    section = lax.axis_index("section")
    return section, section // ROW, section % ROW < DILATION_STRIDE


def coefficients(weights, section):
    at = lax.broadcasted_iota(jnp.int32, weights.shape, 1) == section
    column = jnp.sum(jnp.where(at, weights[...], F32(0.0)), axis=1, keepdims=True)
    return lambda k: column[k : k + 1, :]


def kept(condition, value):
    return jnp.where(condition, value, jnp.zeros_like(value))


def slots_kernel(history, *refs):
    outs, sems = refs[:-1], refs[-1]
    _, _, low = place_in_grid()
    slots = (first_slots()[1], jnp.where(low, 3, 1), 6, 4, 2, 1)
    copies = [
        pltpu.make_async_copy(history.at[slot - 1], out, sems.at[i])
        for i, (slot, out) in enumerate(zip(slots, outs))
    ]
    for copy in copies:
        copy.start()
    for copy in copies:
        copy.wait()


def first_slots():
    _, row, low = place_in_grid()
    return jnp.where(row < 2, jnp.where(low, 5, 3), jnp.where(low, 3, 1)), jnp.where(low, 7, 5)


def weighted(out, first_column, *terms):
    width = out.shape[1]
    for start in range(0, out.shape[0], 16):
        rows = slice(start, start + 16)
        total = None
        for factor, block in terms:
            first = first_column if block.shape[1] > width else 0
            term = block[rows, first : first + width].astype(F32)
            term = term if factor is None else factor * term
            total = term if total is None else total + term
        out[rows, :] = total.astype(out.dtype)


def two_rows_kernel(weights, straight, crossed, *outs):
    section, _, low = place_in_grid()
    factor = coefficients(weights, jnp.minimum(section + 2 * ROW, weights.shape[1] - 1))
    first = 0
    for out in outs:
        weighted(out, first, (factor(4), straight), (jnp.where(low, factor(3), factor(5)), crossed))
        first += out.shape[1]


def one_row(first_column):
    def kernel(weights, straight, crossed_early, crossed_late, carried, out):
        section, row, low = place_in_grid()
        factor = coefficients(weights, jnp.minimum(section + ROW, weights.shape[1] - 1))
        crossed = jnp.where(low, factor(1), factor(3))
        weighted(
            out,
            first_column,
            (factor(2), straight),
            (kept(row == 2, crossed), crossed_early),
            (kept(row < 2, crossed), crossed_late),
            (None, carried),
        )

    return kernel


def projected(rows, wq, joined):
    query = jnp.dot(rows, wq, preferred_element_type=F32).astype(BF16)
    out = jnp.dot(rows, joined, preferred_element_type=F32)
    low = lax.broadcasted_iota(jnp.int32, (1, LANES), 1) < HEAD_DIM
    parts = []
    for start in (0, LANES):
        pair = out[:, start : start + LANES]
        swapped = pltpu.roll(pair, HEAD_DIM, 1)
        zero = jnp.zeros_like(pair)
        parts += [
            jnp.where(low, pair, zero),
            jnp.where(low, zero, swapped),
            jnp.where(low, swapped, zero),
            jnp.where(low, zero, pair),
        ]
    return query, jnp.concatenate([part.astype(BF16) for part in parts], axis=1)


def project_kernel(*refs):
    *blocks, wq, joined, query_ref, kv_ref = refs
    rows = jnp.concatenate([block[...] for block in blocks], axis=0)
    query_ref[...], kv_ref[...] = projected(rows, wq[...], joined[...])


def attended(query, kv, block):
    rows, place, ring = query.shape[0], lax.axis_index("tensor"), len(BLOCK_OFFSETS)
    row = lax.broadcasted_iota(jnp.int32, (rows, 1), 0) + (place + block) % ring * rows
    lane = lax.broadcasted_iota(jnp.int32, (1, rows), 1)
    key = jnp.concatenate([lane + (place + b) % ring * rows for b in BLOCK_OFFSETS], axis=1)
    bias = jnp.where(row >= key, F32(0.0), F32(-1e30))
    low = lax.broadcasted_iota(jnp.int32, (kv.shape[0], LANES), 1) < HEAD_DIM
    ones = [jnp.where(side, F32(1.0), F32(0.0)).astype(BF16) for side in (low, ~low)]
    out = []
    pairs = query.shape[1] // LANES
    for group in range(2):
        keys, values = [], []
        for side in range(2):
            at = (2 * group + side) * LANES
            keys.append(kv[:, at : at + LANES])
            values.append(jnp.concatenate([kv[:, 4 * LANES + at : 5 * LANES + at], ones[side]], axis=1))
        values = jnp.concatenate(values, axis=0)
        for pair in range(group * pairs // 2, (group + 1) * pairs // 2):
            q_pair = query[:, pair * LANES : (pair + 1) * LANES]
            weights = []
            for side in range(2):
                scores = lax.dot_general(q_pair, keys[side], (((1,), (1,)), ((), ())), preferred_element_type=F32)
                scores = scores + bias
                highest = jnp.max(scores, axis=-1, keepdims=True)
                weights.append(jnp.exp2((scores - highest) * F32(HEAD_DIM**-0.5 * LOG2_E)).astype(BF16))
            summed = jnp.dot(jnp.concatenate(weights, axis=1), values, preferred_element_type=F32)
            out.append((summed[:, :LANES] * (1.0 / summed[:, LANES:])).astype(BF16))
    return jnp.concatenate(out, axis=1)


def put_projected(heads, outward, top_ref, bottom_ref):
    half, width = top_ref.shape
    step = PROJECTED_COLUMNS
    for start in range(0, width, step):
        part = jnp.dot(heads, outward[:, start : start + step], preferred_element_type=F32).astype(BF16)
        top_ref[:, start : start + step] = part[:half]
        bottom_ref[:, start : start + step] = part[half:]


def opposite_kernel(top, bottom, wq, joined, kv0, kv1, outward, out_top, out_bottom, kv_ref):
    rows = jnp.concatenate([top[...], bottom[...]], axis=0)
    query, kv3 = projected(rows, wq[...], joined[...])
    kv_ref[...] = kv3
    kv = jnp.concatenate([kv0[...], kv1[...], kv3], axis=0)
    put_projected(attended(query, kv, BLOCK_OFFSETS[3]), outward, out_top, out_bottom)


def sides_kernel(query, kv0, kv1, kv3, outward, left_top, left_bottom, right_top, right_bottom):
    kv = jnp.concatenate([kv0[...], kv1[...], kv3[...]], axis=0)
    rows = query.shape[0] // 2
    put_projected(attended(query[:rows, :], kv, BLOCK_OFFSETS[1]), outward, left_top, left_bottom)
    put_projected(attended(query[rows:, :], kv, BLOCK_OFFSETS[2]), outward, right_top, right_bottom)


def own_kernel(query, kv0, kv1, kv3, outward, top, bottom):
    kv = jnp.concatenate([kv0[...], kv1[...], kv3[...]], axis=0)
    put_projected(attended(query[...], kv, BLOCK_OFFSETS[0]), outward, top, bottom)


def merge_kernel(right_top, left_bottom, from_left, from_right, *outs):
    count, start = len(outs) // 2, 0
    for c in range(count):
        cols = slice(start, start + outs[c].shape[1])
        start = cols.stop
        outs[c][...] = (right_top[:, cols].astype(F32) + from_left[:, cols].astype(F32)).astype(BF16)
        outs[count + c][...] = (left_bottom[:, cols].astype(F32) + from_right[:, cols].astype(F32)).astype(BF16)


def finish(first_column, first_arrived):
    def kernel(weights, tokens, *refs):
        *parts, arrived, straight, crossed, same_row, out = refs
        half = out.shape[0] // 2
        section, row, low = place_in_grid()
        factor = coefficients(weights, section)
        cols = slice(first_column, first_column + out.shape[1])
        there = slice(first_arrived, first_arrived + out.shape[1])
        far, far_odd = kept(row == 3, factor(6)), kept(row == 3, jnp.where(low, factor(5), factor(7)))
        near = kept(jnp.logical_not(low), factor(1))
        for base, (own, plain, merged) in ((0, parts[:3]), (half, parts[3:])):
            for start in range(0, half, 16):
                rows, here = slice(base + start, base + start + 16), slice(start, start + 16)
                attention_sum = own[here, cols].astype(F32) + plain[here, cols].astype(F32)
                attention_sum = attention_sum + merged[here, :].astype(F32)
                block_out = (tokens[rows, cols].astype(F32) + attention_sum).astype(BF16)
                past = arrived[rows, there].astype(F32) + far * straight[rows, cols].astype(F32)
                past = past + far_odd * crossed[rows, cols].astype(F32)
                past = past + near * same_row[rows, cols].astype(F32)
                out[rows, :] = (factor(0) * block_out.astype(F32) + past).astype(BF16)

    return kernel


def store_kernel(*refs):
    *pieces, out, sems = refs
    first, copies = 0, []
    for i, piece in enumerate(pieces):
        last = first + piece.shape[1]
        copies.append(pltpu.make_async_copy(piece, out.at[:, first:last], sems.at[i]))
        first = last
    for copy in copies:
        copy.start()
    for copy in copies:
        copy.wait()


def store_last_kernel(_, piece, out, sems):
    copy = pltpu.make_async_copy(piece, out.at[:, out.shape[1] - piece.shape[1] :], sems.at[0])
    copy.start()
    copy.wait()


def stored(kernel, out, *pieces, aliases):
    specs = [pl.BlockSpec(memory_space=pltpu.VMEM)] * len(pieces)
    if aliases:
        specs[0] = pl.BlockSpec(memory_space=pltpu.HBM)
    return pl.pallas_call(
        kernel,
        out_shape=pltpu.HBM(*out),
        in_specs=specs,
        out_specs=pl.BlockSpec(memory_space=pltpu.HBM),
        scratch_shapes=[pltpu.SemaphoreType.DMA((len(pieces),))],
        input_output_aliases=aliases,
        compiler_params=pltpu.CompilerParams(vmem_limit_bytes=4 * MIB),
    )(*pieces)


def cut(width, proportions):
    return [width * part // sum(proportions) for part in proportions]


def on_device(
    section_input, history, query_weight, key_weight, value_weight, output_weight, mix_weights
):
    token_rows = section_input[0]
    rows, width = token_rows.shape
    half, sizes = rows // 2, cut(width, CARRIED_PIECES)
    wq, wk, wv, wo = query_weight[0], key_weight[0], value_weight[0], output_weight[0]
    q_width = wq.shape[1]
    table = mix_weights.T
    half_block, block, kv_width = ((half, width), BF16), ((rows, width), BF16), 8 * LANES
    rows_of = lambda first, last: range(first * ROW, last * ROW)
    swap = lambda i: DILATION_STRIDE if i % ROW < DILATION_STRIDE else -DILATION_STRIDE

    normed, early = on_chip(
        prologue_kernel, [block] * 2, token_rows, history[0], limit=6,
        scratch=[pltpu.VMEM((rows, width), BF16), pltpu.SemaphoreType.DMA((2,))], spaces=[pltpu.HBM] * 2,
    )
    left, right = around(normed, 1), around(normed, -1)
    opposite_top, opposite_bottom = around(left[:half], 1), around(right[half:], -1)

    pieces_of = [((rows, size), BF16) for size in sizes]
    far, late, far_straight, two_straight, one_straight, same_row = on_chip(
        slots_kernel, [block] * 6, history[0],
        limit=7, scratch=[pltpu.SemaphoreType.DMA((6,))], spaces=[pltpu.HBM],
    )
    crossed_early = sent(early, rows_of(0, 3), swap)
    far_odd = sent(far, rows_of(0, 1), lambda i: 3 * ROW + swap(i))
    crossed_late = sent(late, rows_of(0, 2), swap)
    far_even = sent(far_straight, rows_of(0, 1), lambda i: 3 * ROW)

    two_rows = on_chip(two_rows_kernel, pieces_of, table, two_straight, crossed_early, limit=6)
    carried = [sent(piece, rows_of(0, 2), lambda i: ROW) for piece in two_rows]
    near_row = sent(same_row, [i for i in rows_of(0, 4) if swap(i) > 0], swap)
    arrived = []
    for c, piece in enumerate(pieces_of):
        (summed,) = on_chip(
            one_row(sum(sizes[:c])), [piece],
            table, one_straight, crossed_early, crossed_late, carried[c], limit=6,
        )
        arrived.append(sent(summed, rows_of(0, 3), lambda i: ROW))

    (joined,) = on_chip(
        load_kernel, [((width, 2 * LANES), BF16)], wk, wv,
        limit=3, scratch=[pltpu.SemaphoreType.DMA((2,))], spaces=[pltpu.HBM] * 2,
    )
    q0, kv0 = on_chip(
        project_kernel, [((rows, q_width), BF16), ((rows, kv_width), BF16)], normed, wq, joined,
        limit=12,
    )
    q1, kv1 = on_chip(
        project_kernel, [((2 * rows, q_width), BF16), ((2 * rows, kv_width), BF16)],
        left, right, wq, joined, limit=16,
    )
    out3_top, out3_bottom, kv3 = on_chip(
        opposite_kernel, [half_block, half_block, ((rows, kv_width), BF16)],
        opposite_top, opposite_bottom, wq, joined, kv0, kv1, wo,
    )
    from_left_merge, from_right_merge = around(out3_top, 1), around(out3_bottom, -1)
    left_out_top, left_out_bottom, right_out_top, right_out_bottom = on_chip(
        sides_kernel, [half_block] * 4, q1, kv0, kv1, kv3, wo
    )
    plain_left, plain_right = around(right_out_bottom, 1), around(left_out_top, -1)
    own_top, own_bottom = on_chip(own_kernel, [half_block] * 2, q0, kv0, kv1, kv3, wo)
    merged_sizes, pieces, first = cut(width, MERGED_PIECES), [], 0
    merged = on_chip(
        merge_kernel, [((half, size), BF16) for size in 2 * merged_sizes],
        right_out_top, left_out_bottom, from_left_merge, from_right_merge, limit=8,
    )
    for c, size in enumerate(merged_sizes):
        merged_left = around(merged[c], 1)
        merged_right = around(merged[len(merged_sizes) + c], -1)
        piece = 0 if first + size <= sizes[0] else 1
        (mixed,) = on_chip(
            finish(first, first - sizes[0] * piece), [((rows, size), BF16)], table, token_rows,
            own_top, plain_right, merged_left, own_bottom, plain_left, merged_right,
            arrived[piece], far_even, far_odd, near_row, limit=8,
        )
        pieces.append(to_next_section(mixed))
        first += size
    begun = stored(store_kernel, block, *pieces[:-1], aliases={})
    return stored(store_last_kernel, block, begun, pieces[-1], aliases={0: 0})[None]


def solution(mesh):
    placed = (
        P("section", "tensor", None),
        P("section", None, "tensor", None),
        P("section", None, "tensor"),
        P("section", None, "tensor"),
        P("section", None, "tensor"),
        P("section", "tensor", None),
        P(),
    )

    return jax.shard_map(
        on_device,
        mesh=mesh,
        in_specs=placed,
        out_specs=P("section", "tensor", None),
        check_vma=False,
    )
```
